32 devices in a mesh: exp: 8 (over y, x, core), tp: 4 (over z).
Axes of the slice: x: 2, y: 2, z: 4, core: 2. Of those that a mesh axis runs over, the one named last changes fastest.
Arguments:
- tokens: bfloat16 [224, 4096], P('exp', 'tp'), may hold values from -6 to 6
- cotangent: bfloat16 [224, 4096], P('exp', 'tp'), may hold values from -6 to 6
- experts: int32 [224, 2], P('exp'), may hold values from 0 to 7, all different within a row; in each aligned block of 28 rows (0 to 27, 28 to 55, ...) at most 8 rows name the same one
- gates: float32 [224, 2], P('exp'), may hold values from 0.1 to 0.9
- w_gate: bfloat16 [8, 4096, 8192], P('exp', None, 'tp'), may hold values from -0.09375 to 0.09375
- w_up: bfloat16 [8, 4096, 8192], P('exp', None, 'tp'), may hold values from -0.09375 to 0.09375
- w_down: bfloat16 [8, 8192, 4096], P('exp', 'tp'), may hold values from -0.0625 to 0.0625
Outputs:
- output: bfloat16 [224, 4096], P('exp', 'tp')
- input_grad: bfloat16 [224, 4096], P('exp', 'tp')
- grad_gate: bfloat16 [8, 4096, 8192], P('exp', None, 'tp')
- grad_up: bfloat16 [8, 4096, 8192], P('exp', None, 'tp')
- grad_down: bfloat16 [8, 8192, 4096], P('exp', 'tp')
The draws below stay inside these ranges and needn't reach their ends.
Inputs may be any that keep to these rules, and one draw needn't show every extreme that they name: Each row names 2 different experts. In each aligned block of 28 rows (the rows of one index of exp) no expert is named by more than 8 rows, and in some blocks one is named by exactly 8.
All inputs are finite; a program needn't handle non-finite values.
Results may differ from the reference program's by a relative error of at most 0.017.
Values may be sent and summed in bfloat16 or wider, within the bound.
A program may use at most 192 MiB of HBM per device.

```python
import math
import jax
import jax.numpy as jnp
import numpy as np
from jax import lax

D = 4096
FF = 8192
EXPERTS = 8
TOP = 2
TOK_DEV = 28
CAP = 8
GROUP = 1
TOKENS = 224
N_EXP = 8


def shard_levels(rng, shape, split, low, largest):
    gain = 1.0
    for dim, shards_of in split:
        draws = jax.random.uniform(jax.random.fold_in(jax.random.fold_in(rng, 6), dim), (shards_of,), jnp.float32, low / len(split), largest / len(split))
        gain = gain * jnp.repeat(jnp.exp(draws), shape[dim] // shards_of).reshape((-1,) + (1,) * (len(shape) - 1 - dim))
    return gain


def routed_block(rng, own, number, rows, count, top, most, slope):
    sequence = jax.random.permutation(rng, count)
    crowded, ordinary = load_shares(count, rows * top, most, slope, True), load_shares(count, rows * top, most, slope, False)
    places = jnp.arange(count)

    def named(lengths, turn):
        used = int((lengths > 0).sum())
        fixed = max(1, used // 4)
        moved = fixed + (places - fixed + turn * (used - fixed)) % max(1, count - fixed)
        return jnp.zeros((count,), jnp.int32).at[sequence[jnp.where(places < fixed, places, moved)]].set(jnp.asarray(lengths, jnp.int32))

    lengths = jnp.where(number % 4 == 0, named(crowded, number // 4), named(ordinary, number - number // 4 - 1))
    mixed = jax.random.permutation(jax.random.fold_in(own, 3), count)
    source_of, sink = mixed[0:count // 2 * 2:2], mixed[1:count // 2 * 2:2]
    room = jnp.minimum(lengths[source_of] - 1, most - lengths[sink]) // 2
    room = jnp.where((source_of == sequence[0]) | (sink == sequence[0]) | (lengths[sink] == 0), 0, jnp.maximum(room, 0))
    moved = jax.random.randint(jax.random.fold_in(own, 4), (count // 2,), 0, 1 << 20) % (room + 1)
    lengths = lengths.at[source_of].add(-moved).at[sink].add(moved)
    members = jnp.searchsorted(jnp.cumsum(lengths), jnp.arange(rows * top), side="right").astype(jnp.int32)
    listing = members.reshape(top, rows).T
    listing = listing[jax.random.permutation(jax.random.fold_in(own, 1), rows)]
    turn = jax.random.randint(jax.random.fold_in(own, 2), (rows, 1), 0, top)
    return jnp.take_along_axis(listing, (jnp.arange(top)[None, :] + turn) % top, axis=1)


def load_shares(count, total, bound, lean, full):
    weights = [(1 << 20) // math.isqrt(standing ** lean) + 1 for standing in range(1, count + 1)]
    largest = bound if full else min(bound, max(-(-total // count), total * weights[0] // sum(weights)))
    least = 1 if total - largest >= count - 1 else 0
    counts, rest = [largest] + [least] * (count - 1), total - largest - least * (count - 1)
    while rest > 0:
        free = [i for i in range(1, count) if counts[i] < largest] or [i for i in range(1, count) if counts[i] < bound]
        pool, budget = sum([weights[i] for i in free]), rest
        for i in free:
            more = min(bound - counts[i], max(1, budget * weights[i] // pool), rest)
            counts[i] = counts[i] + more
            rest = rest - more
    return np.array(counts)


def noise(key, extent, spread, most, split=(), kind=jnp.bfloat16):
    entries = jax.random.normal(key, extent, jnp.float32) * spread
    if len(split) > 0:
        entries = shard_levels(key, extent, split, -0.22, 0.18) * entries
    return jnp.clip(entries, min=-most, max=most).astype(kind)


def setup_inputs(seed: int = 0) -> dict:
    streams_of = jax.random.split(jax.random.key(seed), 8)
    tokens = noise(streams_of[0], (TOKENS, D), 1.0, 6.0, ((0, 8), (1, 4)))
    cotangent = noise(streams_of[1], (TOKENS, D), 1.0, 6.0, ((0, 8), (1, 4)))
    experts_keys = jax.random.split(jax.random.fold_in(streams_of[2], 1), TOKENS // TOK_DEV)
    experts_turns = jax.random.permutation(jax.random.fold_in(streams_of[2], 3), TOKENS // TOK_DEV)
    experts = jax.vmap(lambda own, number: routed_block(jax.random.fold_in(streams_of[2], 2), own, number, TOK_DEV, EXPERTS, TOP, CAP, 2))(experts_keys, experts_turns).reshape((TOKENS, TOP))
    gates = jnp.clip(0.1 + 0.79999997 * jax.random.uniform(streams_of[3], (TOKENS, TOP), jnp.float32) ** shard_levels(streams_of[3], (TOKENS, TOP), ((0, 8),), -0.2, 0.2), 0.1, 0.9)
    w_gate = noise(streams_of[4], (N_EXP, D, FF // GROUP), D ** -0.5, 0.09375, ((0, 8), (2, 4)))
    w_up = noise(streams_of[5], (N_EXP, D, FF // GROUP), D ** -0.5, 0.09375, ((0, 8), (2, 4)))
    w_down = noise(streams_of[6], (N_EXP, FF // GROUP, D), FF ** -0.5, 0.0625, ((0, 8), (1, 4)))
    return dict(tokens=tokens, cotangent=cotangent, experts=experts, gates=gates, w_gate=w_gate, w_up=w_up, w_down=w_down)


def slot_places(experts):
    pair_ids = experts.reshape(N_EXP, TOK_DEV * TOP)
    matches = (pair_ids[:, :, None] == jnp.arange(EXPERTS, dtype=jnp.int32)[None, None, :]).astype(jnp.int32)
    before = jnp.cumsum(matches, axis=1) - matches
    slot_ids = jnp.sum(before * matches, axis=2)
    source = jnp.arange(N_EXP, dtype=jnp.int32)[:, None] * CAP
    return (source + slot_ids).reshape(TOKENS * TOP).astype(jnp.int32)


def reference(tokens, cotangent, experts, gates, w_gate, w_up, w_down):
    places = slot_places(experts)
    expert_ids = experts.reshape(TOKENS * TOP).astype(jnp.int32)
    buffer_rows = N_EXP * CAP
    repeated = jnp.repeat(tokens, TOP, axis=0)
    scaled = (gates[:, :, None] * cotangent[:, None, :].astype(jnp.float32)).astype(jnp.bfloat16)
    scaled = scaled.reshape(TOKENS * TOP, D)
    part = FF // GROUP
    gate_all = w_gate.reshape(EXPERTS, GROUP, D, part).transpose(0, 2, 1, 3).reshape(EXPERTS, D, FF)
    up_all = w_up.reshape(EXPERTS, GROUP, D, part).transpose(0, 2, 1, 3).reshape(EXPERTS, D, FF)
    down_all = w_down.reshape(EXPERTS, FF, D)

    def expert_pass(expert):
        targets = jnp.where(expert_ids == expert, places, buffer_rows).astype(jnp.int32)
        token_rows = jnp.zeros((buffer_rows, D), jnp.bfloat16).at[targets].set(repeated, mode="drop")
        cot_rows = jnp.zeros((buffer_rows, D), jnp.bfloat16).at[targets].set(scaled, mode="drop")
        gate_mat = gate_all[expert]
        up_mat = up_all[expert]
        down_mat = down_all[expert]
        hidden_gate = jnp.dot(token_rows, gate_mat, preferred_element_type=jnp.float32)
        hidden_up = jnp.dot(token_rows, up_mat, preferred_element_type=jnp.float32)
        sigmoid_gate = jax.nn.sigmoid(hidden_gate)
        activation = (hidden_gate * sigmoid_gate * hidden_up).astype(jnp.bfloat16)
        out_rows = jnp.dot(activation, down_mat, preferred_element_type=jnp.float32)
        grad_act = jnp.dot(cot_rows, down_mat.T, preferred_element_type=jnp.float32)
        grad_first = (grad_act * hidden_up * sigmoid_gate * (1.0 + hidden_gate * (1.0 - sigmoid_gate))).astype(jnp.bfloat16)
        grad_second = (grad_act * hidden_gate * sigmoid_gate).astype(jnp.bfloat16)
        grad_down = jnp.dot(activation.T, cot_rows, preferred_element_type=jnp.float32).astype(jnp.bfloat16)
        grad_gate = jnp.dot(token_rows.T, grad_first, preferred_element_type=jnp.float32).astype(jnp.bfloat16)
        grad_up = jnp.dot(token_rows.T, grad_second, preferred_element_type=jnp.float32).astype(jnp.bfloat16)
        back_rows = jnp.dot(grad_first, gate_mat.T, preferred_element_type=jnp.float32)
        back_rows = back_rows + jnp.dot(grad_second, up_mat.T, preferred_element_type=jnp.float32)
        return out_rows, back_rows, grad_gate, grad_up, grad_down

    results = lax.map(expert_pass, jnp.arange(EXPERTS, dtype=jnp.int32))
    flat = (expert_ids * buffer_rows + places).astype(jnp.int32)
    out_pairs = results[0].reshape(EXPERTS * buffer_rows, D)[flat].reshape(TOKENS, TOP, D)
    back_pairs = results[1].reshape(EXPERTS * buffer_rows, D)[flat].reshape(TOKENS, TOP, D)
    output = jnp.sum(gates[:, :, None] * out_pairs, axis=1).astype(jnp.bfloat16)
    input_grad = jnp.sum(back_pairs, axis=1).astype(jnp.bfloat16)
    grad_gate = results[2].reshape(EXPERTS, D, GROUP, part).transpose(0, 2, 1, 3).reshape(N_EXP, D, part)
    grad_up = results[3].reshape(EXPERTS, D, GROUP, part).transpose(0, 2, 1, 3).reshape(N_EXP, D, part)
    grad_down = results[4].reshape(N_EXP, part, D)
    return output, input_grad, grad_gate, grad_up, grad_down
```

```python
import functools

import jax
import jax.numpy as jnp
from jax import lax
from jax.experimental import pallas as pl
from jax.experimental.pallas import tpu as pltpu
from jax.sharding import PartitionSpec as P

EXPERTS = 8
CAP = 8
PAIR = 2 * CAP
MESH = pl.DeviceIdType.MESH
LOW = jnp.bfloat16
F32 = jnp.float32


def contract_rows(left, right):
    return lax.dot_general(left, right, (((0,), (0,)), ((), ())), preferred_element_type=F32)


def contract_cols(left, right):
    return lax.dot_general(left, right, (((1,), (1,)), ((), ())), preferred_element_type=F32)


def flip(index, bits):
    out, unit = index, 1
    while unit <= bits:
        if bits & unit:
            out = out + unit * (1 - 2 * ((index // unit) % 2))
        unit *= 2
    return out


def round_up(value, unit):
    return -(-value // unit) * unit


def make_tables(group, experts_ref, gates_ref, table, pick, comb):
    count = experts_ref.shape[0]
    pad = round_up(count, 16)
    lane = lax.broadcasted_iota(jnp.int32, (count, 128), 1)
    ids = [experts_ref[:, j : j + 1] for j in range(2)]
    gates = [gates_ref[:, j : j + 1] for j in range(2)]
    hits = [(ids[j] == lane).astype(F32) for j in range(2)]
    tri = (
        lax.broadcasted_iota(jnp.int32, (count, count), 0)
        > lax.broadcasted_iota(jnp.int32, (count, count), 1)
    ).astype(F32)
    before = jnp.dot(tri, hits[0] + hits[1], preferred_element_type=F32)
    places = [
        ids[j] * CAP + jnp.sum(before * hits[j], axis=1, keepdims=True).astype(jnp.int32)
        for j in range(2)
    ]
    table[...] = jnp.zeros_like(table)
    comb[...] = jnp.zeros_like(comb)

    def columns(width, share):
        col = lax.broadcasted_iota(jnp.int32, (count, width), 1)
        owner = col // (PAIR * share)
        return owner * CAP + col % CAP, (col % PAIR) < CAP

    where, first = columns(EXPERTS * PAIR, 1)
    hit = [places[j] == where for j in range(2)]
    table[0:count, :] = ((hit[0] | hit[1]) & first).astype(F32)
    for j in range(2):
        table[(1 + j) * pad : (1 + j) * pad + count, :] = jnp.where(first, 0.0, hit[j].astype(F32))
    pick[...] = table[...].T.astype(LOW)

    where, first = columns(comb.shape[1], group)
    hit = [(places[j] == where).astype(F32) for j in range(2)]
    weight = jnp.where(first, hit[0] * gates[0] + hit[1] * gates[1], 0.0)
    for part in range(3):
        piece = weight.astype(LOW)
        comb[part * pad : part * pad + count, :] = piece
        weight = weight - piece.astype(F32)
    comb[3 * pad : 3 * pad + count, :] = jnp.where(first, 0.0, hit[0] + hit[1]).astype(LOW)


def forward_kernel(
    n, m, group, bf, bc,
    tok_hbm, cot_hbm, experts_ref, gates_ref, wg_hbm, wu_hbm, wd_hbm,
    x_ref, g_ref, a_ref, d1_ref, d3_ref, out_ref,
    wg, wu, wd, w_sem, tok, t_sem, table, pick, comb, stack, send, held,
    h1_acc, h3_acc, da_acc, back, home, part_send, got,
    sa, ra, sb, rb, sc, rc, sd, rd,
):
    e, t = lax.axis_index("exp"), lax.axis_index("tp")
    count, cols = tok_hbm.shape
    hidden = wg.shape[1]
    pad = round_up(count, 16)
    parts = [flip(t, q) for q in range(m)]

    def cols_of(q):
        return pl.ds(pl.multiple_of(parts[q] * cols, cols), cols)

    def rows_of(device):
        return pl.ds(pl.multiple_of(device * PAIR, PAIR), PAIR)

    own = [
        pltpu.make_async_copy(src, tok.at[0, i], t_sem.at[i])
        for i, src in enumerate((tok_hbm, cot_hbm))
    ]
    for copy in own:
        copy.start()
    barrier = pltpu.get_barrier_semaphore()
    for r in range(1, n):
        pl.semaphore_signal(
            barrier, inc=1, device_id={"exp": lax.rem(e + r, n), "tp": t}, device_id_type=MESH
        )
    for q in range(1, m):
        pl.semaphore_signal(
            barrier, inc=1, device_id={"exp": e, "tp": parts[q]}, device_id_type=MESH
        )
    loads = []
    for q in range(m):
        span = cols_of(q)
        loads.append((
            pltpu.make_async_copy(wg_hbm.at[0, span, :], wg.at[span, :], w_sem.at[q, 0]),
            pltpu.make_async_copy(wu_hbm.at[0, span, :], wu.at[span, :], w_sem.at[q, 1]),
            pltpu.make_async_copy(wd_hbm.at[0, :, span], wd.at[:, span], w_sem.at[q, 2]),
        ))
        for copy in loads[q]:
            copy.start()
    make_tables(group, experts_ref, gates_ref, table, pick, comb)
    stack[...] = jnp.zeros_like(stack)
    for copy in own:
        copy.wait()
    pl.semaphore_wait(barrier, n - 1 + m - 1)

    gather = [None]
    for q in range(1, m):
        gather.append(
            pltpu.make_async_remote_copy(
                src_ref=tok.at[0],
                dst_ref=tok.at[q],
                send_sem=sa.at[q],
                recv_sem=ra.at[q],
                device_id={"exp": e, "tp": parts[q]},
                device_id_type=MESH,
            )
        )
        gather[q].start()

    def to_experts(q, r):
        dest = lax.rem(e + r, n)
        return pltpu.make_async_remote_copy(
            src_ref=send.at[dest // group, :, cols_of(q)],
            dst_ref=held.at[rows_of(e), cols_of(q)],
            send_sem=sb.at[q, r],
            recv_sem=rb.at[q, r],
            device_id={"exp": dest, "tp": t},
            device_id_type=MESH,
        )

    def to_tokens(q, r):
        dest = lax.rem(e + r, n)
        return pltpu.make_async_remote_copy(
            src_ref=back.at[rows_of(dest), cols_of(q)],
            dst_ref=home.at[rows_of(e), cols_of(q)],
            send_sem=sc.at[q, r],
            recv_sem=rc.at[q, r],
            device_id={"exp": dest, "tp": t},
            device_id_type=MESH,
        )

    def to_owner(q):
        return pltpu.make_async_remote_copy(
            src_ref=part_send.at[q],
            dst_ref=got.at[q],
            send_sem=sd.at[q],
            recv_sem=rd.at[q],
            device_id={"exp": e, "tp": parts[q]},
            device_id_type=MESH,
        )

    def dispatch(q):
        if q > 0:
            gather[q].wait_recv()
        stack[0:count, :] = tok[q, 0]
        cot = tok[q, 1].astype(F32)
        for j in range(2):
            stack[(1 + j) * pad : (1 + j) * pad + count, :] = (
                cot * gates_ref[:, j : j + 1]
            ).astype(LOW)
        rows = jnp.dot(pick[...], stack[...], preferred_element_type=F32).astype(LOW)
        send[:, :, cols_of(q)] = rows.reshape(EXPERTS, PAIR, cols)

        @pl.loop(1, n)
        def _(r):
            to_experts(q, r).start()

        held[rows_of(e), cols_of(q)] = send[e // group, :, cols_of(q)]

    def phase_one(q):
        span = cols_of(q)

        @pl.loop(1, n)
        def _(r):
            to_experts(q, r).wait_recv()

        pair = held[:, span].astype(F32).reshape(n, 2, CAP, cols)
        x_ref[:, span] = pair[:, 0].reshape(n * CAP, cols).astype(LOW)
        g_ref[:, span] = pair[:, 1].reshape(n * CAP, cols).astype(LOW)
        for copy in loads[q]:
            copy.wait()

        @pl.loop(0, hidden // bf)
        def _(j):
            units = pl.ds(pl.multiple_of(j * bf, bf), bf)
            x, g = x_ref[:, span], g_ref[:, span]
            h1 = jnp.dot(x, wg[span, units], preferred_element_type=F32)
            h3 = jnp.dot(x, wu[span, units], preferred_element_type=F32)
            da = contract_cols(g, wd[units, span])
            if q == 0:
                h1_acc[:, units] = h1
                h3_acc[:, units] = h3
                da_acc[:, units] = da
            else:
                h1_acc[:, units] += h1
                h3_acc[:, units] += h3
                da_acc[:, units] += da

    def phase_two(q):
        @pl.loop(0, cols // bc)
        def _(j):
            span = pl.ds(pl.multiple_of(parts[q] * cols + j * bc, bc), bc)
            y = jnp.dot(a_ref[...], wd[:, span], preferred_element_type=F32)
            b = contract_cols(d1_ref[...], wg[span, :]) + contract_cols(d3_ref[...], wu[span, :])
            both = jnp.concatenate([y.reshape(n, CAP, bc), b.reshape(n, CAP, bc)], axis=1)
            back[:, span] = both.reshape(n * PAIR, bc).astype(LOW)

        @pl.loop(1, n)
        def _(r):
            to_tokens(q, r).start()

        home[rows_of(e), cols_of(q)] = back[rows_of(e), cols_of(q)]

    def combine(q):
        @pl.loop(1, n)
        def _(r):
            to_tokens(q, r).wait_recv()

        made = jnp.dot(comb[...], home[:, cols_of(q)], preferred_element_type=F32)
        output = made[0:pad] + made[pad : 2 * pad] + made[2 * pad : 3 * pad]
        return output[0:count], made[3 * pad : 3 * pad + count]

    def reduce(q):
        output, grad = combine(q)
        part_send[q, 0] = output.astype(LOW)
        part_send[q, 1] = grad.astype(LOW)
        to_owner(q).start()

    dispatch(0)
    for q in range(1, m):
        dispatch(q)
        phase_one(q - 1)
    phase_one(m - 1)

    @pl.loop(0, hidden // bf)
    def _(j):
        units = pl.ds(pl.multiple_of(j * bf, bf), bf)
        h1, h3, da = h1_acc[:, units], h3_acc[:, units], da_acc[:, units]
        sig = jax.nn.sigmoid(h1)
        a_ref[:, units] = (h1 * sig * h3).astype(LOW)
        d1_ref[:, units] = (da * h3 * sig * (1.0 + h1 * (1.0 - sig))).astype(LOW)
        d3_ref[:, units] = (da * h1 * sig).astype(LOW)

    for q in reversed(range(m)):
        phase_two(q)
        if q + 1 < m:
            reduce(q + 1)
    totals = list(combine(0))
    for q in range(1, m):
        to_owner(q).wait_recv()
        for i in range(2):
            totals[i] = totals[i] + got[q, i].astype(F32)
    for i in range(2):
        out_ref[i] = totals[i].astype(LOW)

    for q in range(1, m):
        gather[q].wait_send()
        to_owner(q).wait_send()
    for q in range(m):
        @pl.loop(1, n)
        def _(r):
            to_experts(q, r).wait_send()
            to_tokens(q, r).wait_send()


def grad_kernel(
    wide, tall, slots,
    x_ref, g_ref, a_ref, d1_ref, d3_ref, sums_ref,
    out_hbm, in_hbm, gate_hbm, up_hbm, down_hbm,
    gate, up, down, sems, o_sem,
):
    width, hidden = x_ref.shape[1], a_ref.shape[1]
    small = [
        pltpu.make_async_copy(sums_ref.at[i], dst, o_sem.at[i])
        for i, dst in enumerate((out_hbm, in_hbm))
    ]
    for copy in small:
        copy.start()

    def wide_copies(r, slot):
        span = pl.ds(pl.multiple_of(r * wide, wide), wide)
        return (
            pltpu.make_async_copy(gate.at[slot], gate_hbm.at[0, span, :], sems.at[slot, 0]),
            pltpu.make_async_copy(up.at[slot], up_hbm.at[0, span, :], sems.at[slot, 1]),
        )

    def tall_copy(r, slot):
        span = pl.ds(pl.multiple_of(r * tall, tall), tall)
        return pltpu.make_async_copy(down.at[slot], down_hbm.at[0, span, :], sems.at[slot, 2])

    steps = width // wide

    @pl.loop(0, steps)
    def _(r):
        slot = lax.rem(r, slots)

        @pl.when(r >= slots)
        def _():
            for copy in wide_copies(r - slots, slot):
                copy.wait()

        span = pl.ds(pl.multiple_of(r * wide, wide), wide)
        gate[slot] = contract_rows(x_ref[:, span], d1_ref[...]).astype(LOW)
        up[slot] = contract_rows(x_ref[:, span], d3_ref[...]).astype(LOW)
        for copy in wide_copies(r, slot):
            copy.start()

    count = hidden // tall

    @pl.loop(0, count)
    def _(r):
        slot = lax.rem(r, slots)

        @pl.when(r >= slots)
        def _():
            tall_copy(r - slots, slot).wait()

        span = pl.ds(pl.multiple_of(r * tall, tall), tall)
        down[slot] = contract_rows(a_ref[:, span], g_ref[...]).astype(LOW)
        tall_copy(r, slot).start()

    for r in range(max(0, steps - slots), steps):
        for copy in wide_copies(r, r % slots):
            copy.wait()
    for r in range(max(0, count - slots), count):
        tall_copy(r, r % slots).wait()
    for copy in small:
        copy.wait()


def per_device(tokens, cotangent, experts, gates, w_gate, w_up, w_down):
    n, m = lax.axis_size("exp"), lax.axis_size("tp")
    group = n // EXPERTS
    count, cols = tokens.shape
    width, hidden = w_gate.shape[1], w_gate.shape[2]
    rows = n * CAP
    pad = round_up(count, 16)
    bf = min(1024, hidden)
    bc = min(512, cols)

    vmem = pl.BlockSpec(memory_space=pltpu.VMEM)
    anyw = pl.BlockSpec(memory_space=pl.ANY)
    shape = jax.ShapeDtypeStruct
    dma = pltpu.SemaphoreType.DMA
    x, g, act, d1, d3, sums = pl.pallas_call(
        functools.partial(forward_kernel, n, m, group, bf, bc),
        out_shape=[shape((rows, width), LOW)] * 2
        + [shape((rows, hidden), LOW)] * 3
        + [shape((2, count, cols), LOW)],
        in_specs=[anyw, anyw, vmem, vmem, anyw, anyw, anyw],
        out_specs=[vmem] * 6,
        scratch_shapes=[
            pltpu.VMEM((width, hidden), LOW),
            pltpu.VMEM((width, hidden), LOW),
            pltpu.VMEM((hidden, width), LOW),
            dma((m, 3)),
            pltpu.VMEM((m, 2, count, cols), LOW),
            dma((2,)),
            pltpu.VMEM((128, EXPERTS * PAIR), F32),
            pltpu.VMEM((EXPERTS * PAIR, 128), LOW),
            pltpu.VMEM((4 * pad, n * PAIR), LOW),
            pltpu.VMEM((128, cols), LOW),
            pltpu.VMEM((EXPERTS, PAIR, width), LOW),
            pltpu.VMEM((n * PAIR, width), LOW),
            pltpu.VMEM((rows, hidden), F32),
            pltpu.VMEM((rows, hidden), F32),
            pltpu.VMEM((rows, hidden), F32),
            pltpu.VMEM((n * PAIR, width), LOW),
            pltpu.VMEM((n * PAIR, width), LOW),
            pltpu.VMEM((m, 2, count, cols), LOW),
            pltpu.VMEM((m, 2, count, cols), LOW),
            dma((m,)), dma((m,)), dma((m, n)), dma((m, n)),
            dma((m, n)), dma((m, n)), dma((m,)), dma((m,)),
        ],
        compiler_params=pltpu.CompilerParams(
            collective_id=0, has_side_effects=True, vmem_limit_bytes=62 * 1024 * 1024
        ),
        cost_estimate=pl.CostEstimate(
            flops=12 * rows * width * hidden,
            bytes_accessed=6 * width * hidden,
            transcendentals=rows * hidden,
        ),
        name="forward",
    )(tokens, cotangent, experts, gates, w_gate, w_up, w_down)

    wide, tall, slots = min(512, width), min(256, hidden), 3
    small = shape((count, cols), LOW)
    return pl.pallas_call(
        functools.partial(grad_kernel, wide, tall, slots),
        out_shape=[small, small]
        + [shape(w_gate.shape, LOW), shape(w_up.shape, LOW), shape(w_down.shape, LOW)],
        in_specs=[vmem] * 6,
        out_specs=[anyw] * 5,
        scratch_shapes=[
            pltpu.VMEM((slots, wide, hidden), LOW),
            pltpu.VMEM((slots, wide, hidden), LOW),
            pltpu.VMEM((slots, tall, width), LOW),
            dma((slots, 3)),
            dma((2,)),
        ],
        compiler_params=pltpu.CompilerParams(vmem_limit_bytes=48 * 1024 * 1024),
        cost_estimate=pl.CostEstimate(
            flops=6 * rows * width * hidden, bytes_accessed=6 * width * hidden, transcendentals=0
        ),
        name="grads",
    )(x, g, act, d1, d3, sums)


def solution(mesh):
    token = P("exp", "tp")
    pair = P("exp", None)
    wide = P("exp", None, "tp")
    tall = P("exp", "tp", None)
    return jax.shard_map(
        per_device,
        mesh=mesh,
        in_specs=(token, token, pair, pair, wide, wide, tall),
        out_specs=(token, token, wide, wide, tall),
        check_vma=False,
    )
```

```python
import functools

import jax
import jax.numpy as jnp
from jax import lax
from jax.experimental import pallas as pl
from jax.experimental.pallas import tpu as pltpu
from jax.sharding import PartitionSpec as P

EXPERTS = 8
CAP = 8
PAIR = 2 * CAP
MESH = pl.DeviceIdType.MESH
LOW = jnp.bfloat16
F32 = jnp.float32


def contract_rows(left, right):
    return lax.dot_general(left, right, (((0,), (0,)), ((), ())), preferred_element_type=F32)


def contract_cols(left, right):
    return lax.dot_general(left, right, (((1,), (1,)), ((), ())), preferred_element_type=F32)


def flip(index, bits):
    out, unit = index, 1
    while unit <= bits:
        if bits & unit:
            out = out + unit * (1 - 2 * ((index // unit) % 2))
        unit *= 2
    return out


def round_up(value, unit):
    return -(-value // unit) * unit


def make_tables(group, count, routes, table, pick, comb):
    pad = round_up(count, 16)
    lane = lax.broadcasted_iota(jnp.int32, (count, 128), 1)
    ids = [routes[0:count, j : j + 1].astype(jnp.int32) for j in range(2)]
    gates = [routes[0:count, 8 + j : 9 + j] for j in range(2)]
    hits = [(ids[j] == lane).astype(F32) for j in range(2)]
    tri = (
        lax.broadcasted_iota(jnp.int32, (count, count), 0)
        > lax.broadcasted_iota(jnp.int32, (count, count), 1)
    ).astype(F32)
    before = jnp.dot(tri, hits[0] + hits[1], preferred_element_type=F32)
    places = [
        ids[j] * CAP + jnp.sum(before * hits[j], axis=1, keepdims=True).astype(jnp.int32)
        for j in range(2)
    ]
    table[...] = jnp.zeros_like(table)
    comb[...] = jnp.zeros_like(comb)

    def columns(width, share):
        col = lax.broadcasted_iota(jnp.int32, (count, width), 1)
        owner = col // (PAIR * share)
        return owner * CAP + col % CAP, (col % PAIR) < CAP

    where, first = columns(EXPERTS * PAIR, 1)
    hit = [places[j] == where for j in range(2)]
    table[0:count, :] = ((hit[0] | hit[1]) & first).astype(F32)
    for j in range(2):
        table[(1 + j) * pad : (1 + j) * pad + count, :] = jnp.where(first, 0.0, hit[j].astype(F32))
    pick[...] = table[...].T.astype(LOW)

    where, first = columns(comb.shape[1], group)
    hit = [(places[j] == where).astype(F32) for j in range(2)]
    weight = jnp.where(first, hit[0] * gates[0] + hit[1] * gates[1], 0.0)
    for part in range(3):
        piece = weight.astype(LOW)
        comb[part * pad : part * pad + count, :] = piece
        weight = weight - piece.astype(F32)
    comb[3 * pad : 3 * pad + count, :] = jnp.where(first, 0.0, hit[0] + hit[1]).astype(LOW)


def forward_kernel(
    n, m, group, split, bf,
    tok_hbm, cot_hbm, experts_hbm, gates_hbm, wg_hbm, wu_hbm, wd_hbm,
    x_hbm, g_hbm, a_hbm, d1_hbm, d3_hbm, out_ref,
    x_ref, g_ref, a_ref, d1_ref, d3_ref, k_sem, ids_in, gates_in, routes, wg, wu, wd, w_sem, tok, t_sem, table, pick, comb, stack, send, held,
    h1_acc, h3_acc, da_acc, back, home, part_send, got,
    sa, ra, sb, rb, rc, sd, rd,
):
    e, t = lax.axis_index("exp"), lax.axis_index("tp")
    count, cols = tok_hbm.shape
    hidden = wg.shape[1]
    pad = round_up(count, 16)
    cw = cols // split
    parts = [flip(t, q) for q in range(m)]
    low = [q & -q for q in range(m)]
    order = [0] + sorted(range(1, m), key=lambda q: (-low[q], q))

    def part_cols(q):
        return pl.ds(pl.multiple_of(parts[q] * cols, cols), cols)

    def cols_of(q, h):
        return pl.ds(pl.multiple_of(parts[q] * cols + h * cw, cw), cw)

    def rows_of(device):
        return pl.ds(pl.multiple_of(device * PAIR, PAIR), PAIR)

    own = [
        pltpu.make_async_copy(
            src.at[:, pl.ds(h * cw, cw)], tok.at[0, h, i], t_sem.at[2 + 2 * h + i]
        )
        for h in range(split)
        for i, src in enumerate((tok_hbm, cot_hbm))
    ]
    routing = [
        pltpu.make_async_copy(experts_hbm, ids_in, t_sem.at[0]),
        pltpu.make_async_copy(gates_hbm, gates_in, t_sem.at[1]),
    ]
    for copy in routing + own:
        copy.start()
    barrier = pltpu.get_barrier_semaphore()
    for r in range(1, n):
        pl.semaphore_signal(
            barrier, inc=1, device_id={"exp": lax.rem(e + r, n), "tp": t}, device_id_type=MESH
        )
    for q in range(1, m):
        pl.semaphore_signal(
            barrier, inc=1, device_id={"exp": e, "tp": parts[q]}, device_id_type=MESH
        )
    loads = {}
    for q in order:
        span = part_cols(q)
        loads[q] = (
            pltpu.make_async_copy(wg_hbm.at[0, span, :], wg.at[span, :], w_sem.at[q, 0]),
            pltpu.make_async_copy(wu_hbm.at[0, span, :], wu.at[span, :], w_sem.at[q, 1]),
            pltpu.make_async_copy(wd_hbm.at[0, :, span], wd.at[:, span], w_sem.at[q, 2]),
        )
        for copy in loads[q]:
            copy.start()
    stack[...] = jnp.zeros_like(stack)
    table[...] = jnp.zeros_like(table)
    for copy in routing:
        copy.wait()
    table[0:2, 0:count] = ids_in[...].astype(F32)
    table[8:10, 0:count] = gates_in[...]
    routes[...] = table[...].T
    make_tables(group, count, routes, table, pick, comb)
    for copy in own:
        copy.wait()
    pl.semaphore_wait(barrier, n - 1 + m - 1)

    def gather(q, h):
        return pltpu.make_async_remote_copy(
            src_ref=tok.at[q - low[q], h],
            dst_ref=tok.at[q, h],
            send_sem=sa.at[q, h],
            recv_sem=ra.at[q, h],
            device_id={"exp": e, "tp": parts[low[q]]},
            device_id_type=MESH,
        )

    def to_experts(q, h, r):
        dest = lax.rem(e + r, n)
        return pltpu.make_async_remote_copy(
            src_ref=send.at[dest // group, :, cols_of(q, h)],
            dst_ref=held.at[rows_of(e), cols_of(q, h)],
            send_sem=sb.at[0],
            recv_sem=rb.at[q, h],
            device_id={"exp": dest, "tp": t},
            device_id_type=MESH,
        )

    def to_tokens(q, h, r):
        dest = lax.rem(e + r, n)
        return pltpu.make_async_remote_copy(
            src_ref=back.at[rows_of(dest), cols_of(q, h)],
            dst_ref=home.at[rows_of(e), cols_of(q, h)],
            send_sem=sb.at[1],
            recv_sem=rc.at[q, h],
            device_id={"exp": dest, "tp": t},
            device_id_type=MESH,
        )

    def to_owner(q, h):
        return pltpu.make_async_remote_copy(
            src_ref=part_send.at[q, h],
            dst_ref=got.at[q, h],
            send_sem=sd.at[q, h],
            recv_sem=rd.at[q, h],
            device_id={"exp": e, "tp": parts[low[q]]},
            device_id_type=MESH,
        )

    def each_peer(start):
        if n <= 8:
            for r in range(1, n):
                start(r)
        else:
            pl.loop(1, n)(start)

    def all_rows(ref, span, sems):
        block = ref.at[0 : (n - 1) * PAIR, span]
        return pltpu.make_async_remote_copy(
            src_ref=block,
            dst_ref=block,
            send_sem=sems,
            recv_sem=sems,
            device_id={"exp": lax.rem(e + 1, n), "tp": t},
            device_id_type=MESH,
        )

    def forward_parts(q, h):
        for child in order[1:]:
            if child - low[child] == q:
                gather(child, h).start()

    def dispatch(q):
        for h in range(split):
            if q > 0:
                gather(q, h).wait_recv()
                forward_parts(q, h)
            stack[0:count, :] = tok[q, h, 0]
            cot = tok[q, h, 1].astype(F32)
            for j in range(2):
                stack[(1 + j) * pad : (1 + j) * pad + count, :] = (
                    cot * routes[0:count, 8 + j : 9 + j]
                ).astype(LOW)
            rows = jnp.dot(pick[...], stack[...], preferred_element_type=F32).astype(LOW)
            send[:, :, cols_of(q, h)] = rows.reshape(EXPERTS, PAIR, cw)

            each_peer(lambda r: to_experts(q, h, r).start())
            held[rows_of(e), cols_of(q, h)] = send[e // group, :, cols_of(q, h)]

    def arrive(q):
        for h in range(split):
            all_rows(held, cols_of(q, h), rb.at[q, h]).wait_recv()
        span = part_cols(q)
        pair = held[:, span].astype(F32).reshape(n, 2, CAP, cols)
        x_ref[:, span] = pair[:, 0].reshape(n * CAP, cols).astype(LOW)
        g_ref[:, span] = pair[:, 1].reshape(n * CAP, cols).astype(LOW)
        for copy in loads[q]:
            copy.wait()

    def phase_one(q, start, stop):
        span = part_cols(q)

        @pl.loop(start, stop)
        def _(j):
            units = pl.ds(pl.multiple_of(j * bf, bf), bf)
            x, g = x_ref[:, span], g_ref[:, span]
            h1 = jnp.dot(x, wg[span, units], preferred_element_type=F32)
            h3 = jnp.dot(x, wu[span, units], preferred_element_type=F32)
            da = contract_cols(g, wd[units, span])
            if q == 0:
                h1_acc[:, units] = h1
                h3_acc[:, units] = h3
                da_acc[:, units] = da
            else:
                h1_acc[:, units] += h1
                h3_acc[:, units] += h3
                da_acc[:, units] += da

    def phase_two(q, h):
        span = cols_of(q, h)
        y = jnp.dot(a_ref[...], wd[:, span], preferred_element_type=F32)
        b = contract_cols(d1_ref[...], wg[span, :]) + contract_cols(d3_ref[...], wu[span, :])
        both = jnp.concatenate([y.reshape(n, CAP, cw), b.reshape(n, CAP, cw)], axis=1)
        back[:, span] = both.reshape(n * PAIR, cw).astype(LOW)

        each_peer(lambda r: to_tokens(q, h, r).start())
        home[rows_of(e), span] = back[rows_of(e), span]

    def combine(q, h):
        all_rows(home, cols_of(q, h), rc.at[q, h]).wait_recv()
        made = jnp.dot(comb[...], home[:, cols_of(q, h)], preferred_element_type=F32)
        output = made[0:pad] + made[pad : 2 * pad] + made[2 * pad : 3 * pad]
        totals = [output[0:count], made[3 * pad : 3 * pad + count]]
        for child in range(m - 1, q, -1):
            if child - low[child] == q:
                to_owner(child, h).wait_recv()
                for i in range(2):
                    totals[i] = totals[i] + got[child, h, i].astype(F32)
        for i in range(2):
            if q > 0:
                part_send[q, h, i] = totals[i].astype(LOW)
            else:
                out_ref[i, :, h * cw : (h + 1) * cw] = totals[i].astype(LOW)
        if q > 0:
            to_owner(q, h).start()

    for h in range(split):
        forward_parts(0, h)
    chunks = hidden // bf
    middle = chunks // 2
    dispatch(order[0])
    dispatch(order[1])
    done = 0
    for i in range(2, m):
        at = order[done]
        if i % 2 == 0:
            arrive(at)
            phase_one(at, 0, middle)
        else:
            phase_one(at, middle, chunks)
            done += 1
        dispatch(order[i])
    for at in order[done:]:
        arrive(at)
        phase_one(at, 0, chunks)

    @pl.loop(0, hidden // bf)
    def _(j):
        units = pl.ds(pl.multiple_of(j * bf, bf), bf)
        h1, h3, da = h1_acc[:, units], h3_acc[:, units], da_acc[:, units]
        sig = jax.nn.sigmoid(h1)
        a_ref[:, units] = (h1 * sig * h3).astype(LOW)
        d1_ref[:, units] = (da * h3 * sig * (1.0 + h1 * (1.0 - sig))).astype(LOW)
        d3_ref[:, units] = (da * h1 * sig).astype(LOW)

    keep = [
        pltpu.make_async_copy(src, dst, k_sem.at[i])
        for i, (src, dst) in enumerate((
            (x_ref, x_hbm), (g_ref, g_hbm), (a_ref, a_hbm), (d1_ref, d1_hbm), (d3_ref, d3_hbm)
        ))
    ]
    for copy in keep:
        copy.start()

    todo = [(q, h) for q in reversed(range(m)) for h in range(split)]
    for i, (q, h) in enumerate(todo):
        phase_two(q, h)
        if i >= 2:
            combine(*todo[i - 2])
    for q, h in todo[-2:]:
        combine(q, h)

    for copy in keep:
        copy.wait()
    for q in range(m):
        for h in range(split):
            if q > 0:
                gather(q, h).wait_send()
                to_owner(q, h).wait_send()

    for i in range(2):
        all_rows(held, pl.ds(0, m * cols), sb.at[i]).wait_send()

def grad_kernel(
    wide, tall, slots,
    x_hbm, d1_hbm, d3_hbm, a_hbm, g_hbm, sums_hbm,
    out_hbm, in_hbm, gate_hbm, up_hbm, down_hbm,
    x_ref, d1_ref, d3_ref, a_ref, g_ref, sums_ref, gate, up, down, i_sem, sems, o_sem,
):
    width, hidden = x_ref.shape[1], a_ref.shape[1]
    small = [
        pltpu.make_async_copy(sums_ref.at[i], dst, o_sem.at[i])
        for i, dst in enumerate((out_hbm, in_hbm))
    ]
    loads = [
        pltpu.make_async_copy(src, dst, i_sem.at[i])
        for i, (src, dst) in enumerate((
            (x_hbm, x_ref), (d1_hbm, d1_ref), (d3_hbm, d3_ref),
            (a_hbm, a_ref), (g_hbm, g_ref), (sums_hbm, sums_ref),
        ))
    ]
    for copy in loads:
        copy.start()

    def copies(which, r, slot):
        kept, hbm, size = (
            (gate, gate_hbm, wide), (up, up_hbm, wide), (down, down_hbm, tall)
        )[which]
        span = pl.ds(pl.multiple_of(r * size, size), size)
        return pltpu.make_async_copy(kept.at[slot], hbm.at[0, span, :], sems.at[slot, which])

    def strip(which, r, left, right, kept, size):
        slot = lax.rem(r, slots)

        @pl.when(r >= slots)
        def _():
            copies(which, r - slots, slot).wait()

        span = pl.ds(pl.multiple_of(r * size, size), size)
        kept[slot] = contract_rows(left[:, span], right[...]).astype(LOW)
        copies(which, r, slot).start()

    for copy in loads[:2]:
        copy.wait()
    steps, count = width // wide, hidden // tall

    @pl.loop(0, steps)
    def _(r):
        strip(0, r, x_ref, d1_ref, gate, wide)

    for copy in loads[2:]:
        copy.wait()
    for copy in small:
        copy.start()

    @pl.loop(0, steps)
    def _(r):
        strip(1, r, x_ref, d3_ref, up, wide)

    @pl.loop(0, count)
    def _(r):
        strip(2, r, a_ref, g_ref, down, tall)

    for which, total in ((0, steps), (1, steps), (2, count)):
        for r in range(max(0, total - slots), total):
            copies(which, r, r % slots).wait()
    for copy in small:
        copy.wait()


def per_device(tokens, cotangent, experts, gates, w_gate, w_up, w_down):
    n, m = lax.axis_size("exp"), lax.axis_size("tp")
    group = n // EXPERTS
    count, cols = tokens.shape
    width, hidden = w_gate.shape[1], w_gate.shape[2]
    rows = n * CAP
    pad = round_up(count, 16)
    bf = min(1024, hidden)
    split = 2

    vmem = pl.BlockSpec(memory_space=pltpu.VMEM)
    anyw = pl.BlockSpec(memory_space=pl.ANY)
    shape = jax.ShapeDtypeStruct
    dma = pltpu.SemaphoreType.DMA
    x, g, act, d1, d3, sums = pl.pallas_call(
        functools.partial(forward_kernel, n, m, group, split, bf),
        out_shape=[shape((rows, width), LOW)] * 2
        + [shape((rows, hidden), LOW)] * 3
        + [shape((2, count, cols), LOW)],
        in_specs=[anyw] * 7,
        out_specs=[anyw] * 5 + [vmem],
        scratch_shapes=[
            pltpu.VMEM((rows, width), LOW),
            pltpu.VMEM((rows, width), LOW),
            pltpu.VMEM((rows, hidden), LOW),
            pltpu.VMEM((rows, hidden), LOW),
            pltpu.VMEM((rows, hidden), LOW),
            dma((5,)),
            pltpu.VMEM((2, count), jnp.int32),
            pltpu.VMEM((2, count), F32),
            pltpu.VMEM((128, 128), F32),
            pltpu.VMEM((width, hidden), LOW),
            pltpu.VMEM((width, hidden), LOW),
            pltpu.VMEM((hidden, width), LOW),
            dma((m, 3)),
            pltpu.VMEM((m, split, 2, count, cols // split), LOW),
            dma((2 + 2 * split,)),
            pltpu.VMEM((128, EXPERTS * PAIR), F32),
            pltpu.VMEM((EXPERTS * PAIR, 128), LOW),
            pltpu.VMEM((4 * pad, n * PAIR), LOW),
            pltpu.VMEM((128, cols // split), LOW),
            pltpu.VMEM((EXPERTS, PAIR, width), LOW),
            pltpu.VMEM((n * PAIR, width), LOW),
            pltpu.VMEM((rows, hidden), F32),
            pltpu.VMEM((rows, hidden), F32),
            pltpu.VMEM((rows, hidden), F32),
            pltpu.VMEM((n * PAIR, width), LOW),
            pltpu.VMEM((n * PAIR, width), LOW),
            pltpu.VMEM((m, split, 2, count, cols // split), LOW),
            pltpu.VMEM((m, split, 2, count, cols // split), LOW),
            dma((m, split)), dma((m, split)), dma((2,)), dma((m, split)),
            dma((m, split)), dma((m, split)), dma((m, split)),
        ],
        compiler_params=pltpu.CompilerParams(
            collective_id=0, has_side_effects=True, vmem_limit_bytes=62 * 1024 * 1024
        ),
        cost_estimate=pl.CostEstimate(
            flops=12 * rows * width * hidden,
            bytes_accessed=6 * width * hidden,
            transcendentals=rows * hidden,
        ),
        name="forward",
    )(tokens, cotangent, experts.T, gates.T, w_gate, w_up, w_down)

    wide, tall, slots = min(1024, width), min(512, hidden), 3
    small = shape((count, cols), LOW)
    return pl.pallas_call(
        functools.partial(grad_kernel, wide, tall, slots),
        out_shape=[small, small]
        + [shape(w_gate.shape, LOW), shape(w_up.shape, LOW), shape(w_down.shape, LOW)],
        in_specs=[anyw] * 6,
        out_specs=[anyw] * 5,
        scratch_shapes=[
            pltpu.VMEM((rows, width), LOW),
            pltpu.VMEM((rows, hidden), LOW),
            pltpu.VMEM((rows, hidden), LOW),
            pltpu.VMEM((rows, hidden), LOW),
            pltpu.VMEM((rows, width), LOW),
            pltpu.VMEM((2, count, cols), LOW),
            pltpu.VMEM((slots, wide, hidden), LOW),
            pltpu.VMEM((slots, wide, hidden), LOW),
            pltpu.VMEM((slots, tall, width), LOW),
            dma((6,)),
            dma((slots, 3)),
            dma((2,)),
        ],
        compiler_params=pltpu.CompilerParams(vmem_limit_bytes=62 * 1024 * 1024),
        cost_estimate=pl.CostEstimate(
            flops=6 * rows * width * hidden, bytes_accessed=6 * width * hidden, transcendentals=0
        ),
        name="grads",
    )(x, d1, d3, act, g, sums)


def solution(mesh):
    token = P("exp", "tp")
    pair = P("exp", None)
    wide = P("exp", None, "tp")
    tall = P("exp", "tp", None)
    return jax.shard_map(
        per_device,
        mesh=mesh,
        in_specs=(token, token, pair, pair, wide, wide, tall),
        out_specs=(token, token, wide, wide, tall),
        check_vma=False,
    )
```

```python
import functools

import jax
import jax.numpy as jnp
from jax import lax
from jax.experimental import pallas as pl
from jax.experimental.pallas import tpu as pltpu
from jax.sharding import PartitionSpec as P

EXPERTS = 8
CAP = 8
PAIR = 2 * CAP
MESH = pl.DeviceIdType.MESH
LOW = jnp.bfloat16
F32 = jnp.float32


def contract_rows(left, right):
    return lax.dot_general(left, right, (((0,), (0,)), ((), ())), preferred_element_type=F32)


def contract_cols(left, right):
    return lax.dot_general(left, right, (((1,), (1,)), ((), ())), preferred_element_type=F32)


def flip(index, bits):
    out, unit = index, 1
    while unit <= bits:
        if bits & unit:
            out = out + unit * (1 - 2 * ((index // unit) % 2))
        unit *= 2
    return out


def round_up(value, unit):
    return -(-value // unit) * unit


def make_tables(group, count, routes, table, pick, comb):
    pad = round_up(count, 16)
    lane = lax.broadcasted_iota(jnp.int32, (count, 128), 1)
    ids = [routes[0:count, j : j + 1].astype(jnp.int32) for j in range(2)]
    gates = [routes[0:count, 8 + j : 9 + j] for j in range(2)]
    hits = [(ids[j] == lane).astype(F32) for j in range(2)]
    tri = (
        lax.broadcasted_iota(jnp.int32, (count, count), 0)
        > lax.broadcasted_iota(jnp.int32, (count, count), 1)
    ).astype(F32)
    before = jnp.dot(tri, hits[0] + hits[1], preferred_element_type=F32)
    places = [
        ids[j] * CAP + jnp.sum(before * hits[j], axis=1, keepdims=True).astype(jnp.int32)
        for j in range(2)
    ]
    table[...] = jnp.zeros_like(table)
    comb[...] = jnp.zeros_like(comb)

    def columns(width, share):
        col = lax.broadcasted_iota(jnp.int32, (count, width), 1)
        owner = col // (PAIR * share)
        return owner * CAP + col % CAP, (col % PAIR) < CAP

    where, first = columns(EXPERTS * PAIR, 1)
    hit = [places[j] == where for j in range(2)]
    table[0:count, :] = ((hit[0] | hit[1]) & first).astype(F32)
    for j in range(2):
        table[(1 + j) * pad : (1 + j) * pad + count, :] = jnp.where(first, 0.0, hit[j].astype(F32))
    pick[...] = table[...].T.astype(LOW)

    where, first = columns(comb.shape[1], group)
    hit = [(places[j] == where).astype(F32) for j in range(2)]
    weight = jnp.where(first, hit[0] * gates[0] + hit[1] * gates[1], 0.0)
    for part in range(3):
        piece = weight.astype(LOW)
        comb[part * pad : part * pad + count, :] = piece
        weight = weight - piece.astype(F32)
    comb[3 * pad : 3 * pad + count, :] = jnp.where(first, 0.0, hit[0] + hit[1]).astype(LOW)


def forward_kernel(
    n, m, group, split, bf,
    tok_hbm, cot_hbm, experts_hbm, gates_hbm, wg_hbm, wu_hbm, wd_hbm,
    x_hbm, g_hbm, a_hbm, d1_hbm, d3_hbm, out_ref,
    x_ref, g_ref, a_ref, d1_ref, d3_ref, k_sem, ids_in, gates_in, routes, wg, wu, wd, w_sem, tok, t_sem, table, pick, comb, stack, send, held,
    h1_acc, h3_acc, da_acc, back, home, part_send, got,
    sa, ra, sb, rb, rc, sd, rd,
):
    e, t = lax.axis_index("exp"), lax.axis_index("tp")
    count, cols = tok_hbm.shape
    hidden = wg.shape[1]
    pad = round_up(count, 16)
    cw = cols // split
    parts = [flip(t, q) for q in range(m)]
    low = [q & -q for q in range(m)]
    order = [0] + sorted(range(1, m), key=lambda q: (-low[q], q))

    def part_cols(q):
        return pl.ds(pl.multiple_of(parts[q] * cols, cols), cols)

    def cols_of(q, h):
        return pl.ds(pl.multiple_of(parts[q] * cols + h * cw, cw), cw)

    def rows_of(device):
        return pl.ds(pl.multiple_of(device * PAIR, PAIR), PAIR)

    own = [
        pltpu.make_async_copy(
            src.at[:, pl.ds(h * cw, cw)], tok.at[0, h, i], t_sem.at[2 + 2 * h + i]
        )
        for h in range(split)
        for i, src in enumerate((tok_hbm, cot_hbm))
    ]
    routing = [
        pltpu.make_async_copy(experts_hbm, ids_in, t_sem.at[0]),
        pltpu.make_async_copy(gates_hbm, gates_in, t_sem.at[1]),
    ]
    for copy in routing + own:
        copy.start()
    barrier = pltpu.get_barrier_semaphore()
    for r in range(1, n):
        pl.semaphore_signal(
            barrier, inc=1, device_id={"exp": lax.rem(e + r, n), "tp": t}, device_id_type=MESH
        )
    for q in range(1, m):
        pl.semaphore_signal(
            barrier, inc=1, device_id={"exp": e, "tp": parts[q]}, device_id_type=MESH
        )
    loads = {}
    for q in order:
        span = part_cols(q)
        loads[q] = (
            pltpu.make_async_copy(wg_hbm.at[0, span, :], wg.at[span, :], w_sem.at[q, 0]),
            pltpu.make_async_copy(wu_hbm.at[0, span, :], wu.at[span, :], w_sem.at[q, 1]),
            pltpu.make_async_copy(wd_hbm.at[0, :, span], wd.at[:, span], w_sem.at[q, 2]),
        )
        for copy in loads[q]:
            copy.start()
    stack[...] = jnp.zeros_like(stack)
    table[...] = jnp.zeros_like(table)
    for copy in routing:
        copy.wait()
    table[0:2, 0:count] = ids_in[...].astype(F32)
    table[8:10, 0:count] = gates_in[...]
    routes[...] = table[...].T
    make_tables(group, count, routes, table, pick, comb)
    for copy in own:
        copy.wait()
    pl.semaphore_wait(barrier, n - 1 + m - 1)

    def gather(q, h):
        return pltpu.make_async_remote_copy(
            src_ref=tok.at[q - low[q], h],
            dst_ref=tok.at[q, h],
            send_sem=sa.at[q, h],
            recv_sem=ra.at[q, h],
            device_id={"exp": e, "tp": parts[low[q]]},
            device_id_type=MESH,
        )

    def to_experts(q, h, r):
        dest = lax.rem(e + r, n)
        return pltpu.make_async_remote_copy(
            src_ref=send.at[dest // group, :, cols_of(q, h)],
            dst_ref=held.at[rows_of(e), cols_of(q, h)],
            send_sem=sb.at[0],
            recv_sem=rb.at[q, h],
            device_id={"exp": dest, "tp": t},
            device_id_type=MESH,
        )

    def to_tokens(q, h, r):
        dest = lax.rem(e + r, n)
        return pltpu.make_async_remote_copy(
            src_ref=back.at[rows_of(dest), cols_of(q, h)],
            dst_ref=home.at[rows_of(e), cols_of(q, h)],
            send_sem=sb.at[1],
            recv_sem=rc.at[q, h],
            device_id={"exp": dest, "tp": t},
            device_id_type=MESH,
        )

    def to_owner(q, h):
        return pltpu.make_async_remote_copy(
            src_ref=part_send.at[q, h],
            dst_ref=got.at[q, h],
            send_sem=sd.at[q, h],
            recv_sem=rd.at[q, h],
            device_id={"exp": e, "tp": parts[low[q]]},
            device_id_type=MESH,
        )

    def each_peer(start):
        if n <= 8:
            for r in range(1, n):
                start(r)
        else:
            pl.loop(1, n)(start)

    def all_rows(ref, span, sems):
        block = ref.at[0 : (n - 1) * PAIR, span]
        return pltpu.make_async_remote_copy(
            src_ref=block,
            dst_ref=block,
            send_sem=sems,
            recv_sem=sems,
            device_id={"exp": lax.rem(e + 1, n), "tp": t},
            device_id_type=MESH,
        )

    def forward_parts(q, halves):
        for child in order[1:]:
            if child - low[child] == q:
                for h in halves:
                    gather(child, h).start()

    def dispatch(q):
        for h in range(split):
            if q > 0:
                gather(q, h).wait_recv()
                forward_parts(q, [h])
            stack[0:count, :] = tok[q, h, 0]
            cot = tok[q, h, 1].astype(F32)
            for j in range(2):
                stack[(1 + j) * pad : (1 + j) * pad + count, :] = (
                    cot * routes[0:count, 8 + j : 9 + j]
                ).astype(LOW)
            rows = jnp.dot(pick[...], stack[...], preferred_element_type=F32).astype(LOW)
            send[:, :, cols_of(q, h)] = rows.reshape(EXPERTS, PAIR, cw)

            each_peer(lambda r: to_experts(q, h, r).start())
            held[rows_of(e), cols_of(q, h)] = send[e // group, :, cols_of(q, h)]

    def arrive(q):
        for h in range(split):
            all_rows(held, cols_of(q, h), rb.at[q, h]).wait_recv()
        span = part_cols(q)
        pair = held[:, span].astype(F32).reshape(n, 2, CAP, cols)
        x_ref[:, span] = pair[:, 0].reshape(n * CAP, cols).astype(LOW)
        g_ref[:, span] = pair[:, 1].reshape(n * CAP, cols).astype(LOW)
        for copy in loads[q]:
            copy.wait()

    def phase_one(q, start, stop):
        span = part_cols(q)

        @pl.loop(start, stop)
        def _(j):
            units = pl.ds(pl.multiple_of(j * bf, bf), bf)
            x, g = x_ref[:, span], g_ref[:, span]
            h1 = jnp.dot(x, wg[span, units], preferred_element_type=F32)
            h3 = jnp.dot(x, wu[span, units], preferred_element_type=F32)
            da = contract_cols(g, wd[units, span])
            if q == 0:
                h1_acc[:, units] = h1
                h3_acc[:, units] = h3
                da_acc[:, units] = da
            else:
                h1_acc[:, units] += h1
                h3_acc[:, units] += h3
                da_acc[:, units] += da

    def phase_two(q, h):
        span = cols_of(q, h)
        y = jnp.dot(a_ref[...], wd[:, span], preferred_element_type=F32)
        b = contract_cols(d1_ref[...], wg[span, :]) + contract_cols(d3_ref[...], wu[span, :])
        both = jnp.concatenate([y.reshape(n, CAP, cw), b.reshape(n, CAP, cw)], axis=1)
        back[:, span] = both.reshape(n * PAIR, cw).astype(LOW)

        each_peer(lambda r: to_tokens(q, h, r).start())
        home[rows_of(e), span] = back[rows_of(e), span]

    def combine(q, h):
        all_rows(home, cols_of(q, h), rc.at[q, h]).wait_recv()
        made = jnp.dot(comb[...], home[:, cols_of(q, h)], preferred_element_type=F32)
        output = made[0:pad] + made[pad : 2 * pad] + made[2 * pad : 3 * pad]
        totals = [output[0:count], made[3 * pad : 3 * pad + count]]
        for child in range(m - 1, q, -1):
            if child - low[child] == q:
                to_owner(child, h).wait_recv()
                for i in range(2):
                    totals[i] = totals[i] + got[child, h, i].astype(F32)
        for i in range(2):
            if q > 0:
                part_send[q, h, i] = totals[i].astype(LOW)
            else:
                out_ref[i, :, h * cw : (h + 1) * cw] = totals[i].astype(LOW)
        if q > 0:
            to_owner(q, h).start()

    forward_parts(0, range(split))
    chunks = hidden // bf
    middle = chunks // 2
    dispatch(order[0])
    dispatch(order[1])
    done = 0
    for i in range(2, m):
        at = order[done]
        if i % 2 == 0:
            arrive(at)
            phase_one(at, 0, middle)
        else:
            phase_one(at, middle, chunks)
            done += 1
        dispatch(order[i])
    for at in order[done:]:
        arrive(at)
        phase_one(at, 0, chunks)

    @pl.loop(0, hidden // bf)
    def _(j):
        units = pl.ds(pl.multiple_of(j * bf, bf), bf)
        h1, h3, da = h1_acc[:, units], h3_acc[:, units], da_acc[:, units]
        sig = jax.nn.sigmoid(h1)
        a_ref[:, units] = (h1 * sig * h3).astype(LOW)
        d1_ref[:, units] = (da * h3 * sig * (1.0 + h1 * (1.0 - sig))).astype(LOW)
        d3_ref[:, units] = (da * h1 * sig).astype(LOW)

    keep = [
        pltpu.make_async_copy(src, dst, k_sem.at[i])
        for i, (src, dst) in enumerate((
            (x_ref, x_hbm), (g_ref, g_hbm), (a_ref, a_hbm), (d1_ref, d1_hbm), (d3_ref, d3_hbm)
        ))
    ]
    for copy in keep:
        copy.start()

    todo = [(q, h) for q in reversed(range(m)) for h in range(split)]
    for i, (q, h) in enumerate(todo):
        phase_two(q, h)
        if i >= 2:
            combine(*todo[i - 2])
    for q, h in todo[-2:]:
        combine(q, h)

    for copy in keep:
        copy.wait()
    for q in range(m):
        for h in range(split):
            if q > 0:
                gather(q, h).wait_send()
                to_owner(q, h).wait_send()

    for i in range(2):
        all_rows(held, pl.ds(0, m * cols), sb.at[i]).wait_send()

def grad_kernel(
    wide, tall, slots,
    x_hbm, d1_hbm, d3_hbm, a_hbm, g_hbm, sums_hbm,
    out_hbm, in_hbm, gate_hbm, up_hbm, down_hbm,
    x_ref, d1_ref, d3_ref, a_ref, g_ref, sums_ref, gate, up, down, i_sem, sems, o_sem,
):
    width, hidden = x_ref.shape[1], a_ref.shape[1]
    small = [
        pltpu.make_async_copy(sums_ref.at[i], dst, o_sem.at[i])
        for i, dst in enumerate((out_hbm, in_hbm))
    ]
    loads = [
        pltpu.make_async_copy(src, dst, i_sem.at[i])
        for i, (src, dst) in enumerate((
            (x_hbm, x_ref), (d1_hbm, d1_ref), (d3_hbm, d3_ref),
            (a_hbm, a_ref), (g_hbm, g_ref), (sums_hbm, sums_ref),
        ))
    ]
    for copy in loads:
        copy.start()

    def copies(which, r, slot):
        kept, hbm, size = (
            (gate, gate_hbm, wide), (up, up_hbm, wide), (down, down_hbm, tall)
        )[which]
        span = pl.ds(pl.multiple_of(r * size, size), size)
        return pltpu.make_async_copy(kept.at[slot], hbm.at[0, span, :], sems.at[slot, which])

    def strip(which, r, left, right, kept, size):
        slot = lax.rem(r, slots)

        @pl.when(r >= slots)
        def _():
            copies(which, r - slots, slot).wait()

        span = pl.ds(pl.multiple_of(r * size, size), size)
        kept[slot] = contract_rows(left[:, span], right[...]).astype(LOW)
        copies(which, r, slot).start()

    for copy in loads[:2]:
        copy.wait()
    steps, count = width // wide, hidden // tall

    @pl.loop(0, steps)
    def _(r):
        strip(0, r, x_ref, d1_ref, gate, wide)

    for copy in loads[2:]:
        copy.wait()
    for copy in small:
        copy.start()

    @pl.loop(0, steps)
    def _(r):
        strip(1, r, x_ref, d3_ref, up, wide)

    @pl.loop(0, count)
    def _(r):
        strip(2, r, a_ref, g_ref, down, tall)

    for which, total in ((0, steps), (1, steps), (2, count)):
        for r in range(max(0, total - slots), total):
            copies(which, r, r % slots).wait()
    for copy in small:
        copy.wait()


def per_device(tokens, cotangent, experts, gates, w_gate, w_up, w_down):
    n, m = lax.axis_size("exp"), lax.axis_size("tp")
    group = n // EXPERTS
    count, cols = tokens.shape
    width, hidden = w_gate.shape[1], w_gate.shape[2]
    rows = n * CAP
    pad = round_up(count, 16)
    bf = min(2048, hidden)
    split = 2

    vmem = pl.BlockSpec(memory_space=pltpu.VMEM)
    anyw = pl.BlockSpec(memory_space=pl.ANY)
    shape = jax.ShapeDtypeStruct
    dma = pltpu.SemaphoreType.DMA
    x, g, act, d1, d3, sums = pl.pallas_call(
        functools.partial(forward_kernel, n, m, group, split, bf),
        out_shape=[shape((rows, width), LOW)] * 2
        + [shape((rows, hidden), LOW)] * 3
        + [shape((2, count, cols), LOW)],
        in_specs=[anyw] * 7,
        out_specs=[anyw] * 5 + [vmem],
        scratch_shapes=[
            pltpu.VMEM((rows, width), LOW),
            pltpu.VMEM((rows, width), LOW),
            pltpu.VMEM((rows, hidden), LOW),
            pltpu.VMEM((rows, hidden), LOW),
            pltpu.VMEM((rows, hidden), LOW),
            dma((5,)),
            pltpu.VMEM((2, count), jnp.int32),
            pltpu.VMEM((2, count), F32),
            pltpu.VMEM((128, 128), F32),
            pltpu.VMEM((width, hidden), LOW),
            pltpu.VMEM((width, hidden), LOW),
            pltpu.VMEM((hidden, width), LOW),
            dma((m, 3)),
            pltpu.VMEM((m, split, 2, count, cols // split), LOW),
            dma((2 + 2 * split,)),
            pltpu.VMEM((128, EXPERTS * PAIR), F32),
            pltpu.VMEM((EXPERTS * PAIR, 128), LOW),
            pltpu.VMEM((4 * pad, n * PAIR), LOW),
            pltpu.VMEM((128, cols // split), LOW),
            pltpu.VMEM((EXPERTS, PAIR, width), LOW),
            pltpu.VMEM((n * PAIR, width), LOW),
            pltpu.VMEM((rows, hidden), F32),
            pltpu.VMEM((rows, hidden), F32),
            pltpu.VMEM((rows, hidden), F32),
            pltpu.VMEM((n * PAIR, width), LOW),
            pltpu.VMEM((n * PAIR, width), LOW),
            pltpu.VMEM((m, split, 2, count, cols // split), LOW),
            pltpu.VMEM((m, split, 2, count, cols // split), LOW),
            dma((m, split)), dma((m, split)), dma((2,)), dma((m, split)),
            dma((m, split)), dma((m, split)), dma((m, split)),
        ],
        compiler_params=pltpu.CompilerParams(
            collective_id=0, has_side_effects=True, vmem_limit_bytes=62 * 1024 * 1024
        ),
        cost_estimate=pl.CostEstimate(
            flops=12 * rows * width * hidden,
            bytes_accessed=6 * width * hidden,
            transcendentals=rows * hidden,
        ),
        name="forward",
    )(tokens, cotangent, experts.T, gates.T, w_gate, w_up, w_down)

    wide, tall, slots = min(1024, width), min(512, hidden), 3
    small = shape((count, cols), LOW)
    return pl.pallas_call(
        functools.partial(grad_kernel, wide, tall, slots),
        out_shape=[small, small]
        + [shape(w_gate.shape, LOW), shape(w_up.shape, LOW), shape(w_down.shape, LOW)],
        in_specs=[anyw] * 6,
        out_specs=[anyw] * 5,
        scratch_shapes=[
            pltpu.VMEM((rows, width), LOW),
            pltpu.VMEM((rows, hidden), LOW),
            pltpu.VMEM((rows, hidden), LOW),
            pltpu.VMEM((rows, hidden), LOW),
            pltpu.VMEM((rows, width), LOW),
            pltpu.VMEM((2, count, cols), LOW),
            pltpu.VMEM((slots, wide, hidden), LOW),
            pltpu.VMEM((slots, wide, hidden), LOW),
            pltpu.VMEM((slots, tall, width), LOW),
            dma((6,)),
            dma((slots, 3)),
            dma((2,)),
        ],
        compiler_params=pltpu.CompilerParams(vmem_limit_bytes=62 * 1024 * 1024),
        cost_estimate=pl.CostEstimate(
            flops=6 * rows * width * hidden, bytes_accessed=6 * width * hidden, transcendentals=0
        ),
        name="grads",
    )(x, d1, d3, act, g, sums)


def solution(mesh):
    token = P("exp", "tp")
    pair = P("exp", None)
    wide = P("exp", None, "tp")
    tall = P("exp", "tp", None)
    return jax.shard_map(
        per_device,
        mesh=mesh,
        in_specs=(token, token, pair, pair, wide, wide, tall),
        out_specs=(token, token, wide, wide, tall),
        check_vma=False,
    )
```
